32 devices in a mesh: chan: 4 (over y, x), tm: 8 (over z, core).
Axes of the slice: x: 2, y: 2, z: 4, core: 2. Of those that a mesh axis runs over, the one named last changes fastest.
Arguments:
- strain: float32 [768, 131072], P('chan', 'tm'), may hold values from -6 to 6
Outputs:
- power: float32 [768, 8192], P('chan', 'tm')
- nyquist: float32 [768], P('chan')
- mean_power: float32 [8192], P('tm')
The draws below stay inside these ranges and needn't reach their ends.
All inputs are finite; a program needn't handle non-finite values.
Results may differ from the reference program's by a relative error of at most 0.00007.
Values sent between devices are 32-bit elements; how exact they have to be, the bound alone decides.
A program may use at most 192 MiB of HBM per device.

```python
import jax
import jax.numpy as jnp
from jax import lax

SEG = 16384
HOP = 8192
BINS = 8192
CHANNELS = 768
SAMPLES = 131072
SEGMENTS = 15


def level_of(stream_key, extent, split, low, top_value):
    loudness = 1.0
    for dim, shards_of in split:
        draws = jax.random.uniform(jax.random.fold_in(jax.random.fold_in(stream_key, 6), dim), (shards_of,), jnp.float32, low / len(split), top_value / len(split))
        loudness = loudness * jnp.repeat(jnp.exp(draws), extent[dim] // shards_of).reshape((-1,) + (1,) * (len(extent) - 1 - dim))
    return loudness


def bell_draw(key, dims, spread, most, cuts=(), kind=jnp.bfloat16):
    drawn = jax.random.normal(key, dims, jnp.float32) * spread
    if len(cuts) > 0:
        drawn = level_of(key, dims, cuts, -0.22, 0.18) * drawn
    return jnp.clip(drawn, min=-most, max=most).astype(kind)


def setup_inputs(seed: int = 0) -> dict:
    keys = jax.random.split(jax.random.key(seed), 2)
    strain = bell_draw(keys[0], (CHANNELS, SAMPLES), 1.0, 6.0, ((0, 4), (1, 8)), jnp.float32)
    return dict(strain=strain)


def hann_window():
    sample_pos = jnp.arange(SEG, dtype=jnp.float32)
    return 0.5 - 0.5 * jnp.cos(2.0 * jnp.pi * sample_pos / SEG)


def reference(strain):
    window = hann_window()
    energy = jnp.sum(window * window)

    def one_channel(signal):
        blocks = signal.reshape(SEGMENTS + 1, HOP)
        pieces = jnp.concatenate([blocks[:-1], blocks[1:]], axis=1)
        centred = (pieces - jnp.mean(pieces, axis=1, keepdims=True)) * window
        spectrum = jnp.fft.rfft(centred, axis=1)
        return jnp.sum(jnp.real(spectrum) ** 2 + jnp.imag(spectrum) ** 2, axis=0)

    totals = lax.map(one_channel, strain)
    doubling = jnp.where(jnp.arange(BINS) == 0, 1.0, 2.0).astype(totals.dtype)
    power = totals[:, :BINS] * doubling / (SEGMENTS * energy)
    nyquist = totals[:, BINS] / (SEGMENTS * energy)
    mean_power = jnp.mean(power, axis=0)
    return power, nyquist, mean_power
```

```python
import functools

import jax
import jax.numpy as jnp
import numpy as np
from jax import lax
from jax.experimental import pallas as pl
from jax.experimental.pallas import tpu as pltpu
from jax.sharding import PartitionSpec as P

ROOT = 128
HALF = ROOT // 2
ROWS = 8


def split_np(table):
    table = table.astype(np.float32)
    high = table.astype(jnp.bfloat16)
    low = (table - high.astype(np.float32)).astype(jnp.bfloat16)
    return high, low


@functools.cache
def tables(tm_count):
    pos = np.arange(ROOT)
    short = 2.0 * np.pi * (np.outer(pos, pos) % ROOT) / ROOT
    cos_s, sin_s = np.cos(short), np.sin(short)
    first = np.concatenate([cos_s[:HALF], -sin_s[:HALF]], axis=0)
    first_hi, first_lo = split_np(first)
    first_all = np.concatenate(
        [
            np.concatenate([first_hi, first_hi], axis=1),
            np.concatenate([first_lo, first_lo], axis=1),
        ],
        axis=0,
    )
    bands = np.arange(HALF).reshape(tm_count, HALF // tm_count)
    order = np.concatenate([bands, ROOT - 1 - bands], axis=1).reshape(-1)
    cos_o, sin_o = cos_s[:, order], sin_s[:, order]
    second = np.concatenate(
        [np.concatenate([cos_o, -sin_o], axis=1), np.concatenate([sin_o, cos_o], axis=1)], axis=0
    )
    second_hi, second_lo = split_np(second)
    second_all = np.concatenate([second_hi, second_hi, second_lo], axis=0)
    long = 2.0 * np.pi * np.outer(np.arange(HALF + ROWS), pos) / (ROOT * ROOT)
    twist = np.concatenate([np.cos(long), np.sin(long)], axis=1).astype(np.float32)
    seg_len = ROOT * ROOT
    window = 0.5 - 0.5 * np.cos(2.0 * np.pi * np.arange(seg_len) / seg_len)
    energy = float(np.sum(window * window))
    return first_all, second_all, twist, window.reshape(ROOT, ROOT).astype(np.float32), energy


def split(value):
    high = value.astype(jnp.bfloat16)
    low = (value - high.astype(jnp.float32)).astype(jnp.bfloat16)
    return high, low


def stage_one(parts, window_ref, first_ref, twist_ref, buf, zbuf, ebuf, row, erow):
    half_len = ROOT * HALF
    total = jnp.zeros((ROWS, ROOT), jnp.float32)
    for ref, offset in parts:
        total = total + jnp.sum(
            jnp.stack([ref[:, offset + ROOT * a : offset + ROOT * (a + 1)] for a in range(HALF)]), axis=0
        )
    mean = jnp.sum(total, axis=1, keepdims=True) * (1.0 / (2 * half_len))
    mean = jnp.broadcast_to(mean, (ROWS, ROOT))
    even = jnp.zeros((ROWS, ROOT), jnp.float32)
    odd = jnp.zeros((ROWS, ROOT), jnp.float32)
    for a in range(ROOT):
        ref, offset = parts[a // HALF]
        start = offset + ROOT * (a % HALF)
        tile = (ref[:, start : start + ROOT] - mean) * window_ref[a : a + 1, :]
        buf[ROWS * a : ROWS * (a + 1), :] = tile
        if a % 2 == 0:
            even = even + tile
        else:
            odd = odd + tile
    alt = even - odd
    sign = (1 - 2 * (lax.broadcasted_iota(jnp.int32, (ROWS, ROOT), 1) % 2)).astype(jnp.float32)
    edge = jnp.sum((even + odd) * sign, axis=1, keepdims=True)
    turn = twist_ref[HALF : HALF + 1, :]
    high, low = split(jnp.concatenate([alt * turn[:, :ROOT], -alt * turn[:, ROOT:]], axis=1))
    ebuf[erow : erow + ROWS, :] = jnp.concatenate([high, low, high], axis=1)
    cos_t, sin_t = twist_ref[:HALF, :ROOT], twist_ref[:HALF, ROOT:]
    for r in range(0, ROWS, 2):
        pair = jnp.concatenate(
            [buf[pl.ds(r, ROOT, stride=ROWS), :], buf[pl.ds(r + 1, ROOT, stride=ROWS), :]], axis=1
        )
        high, low = split(pair)
        out = jnp.dot(
            first_ref[...], jnp.concatenate([high, low], axis=0), preferred_element_type=jnp.float32
        )
        out = out[:ROOT] + out[ROOT:]
        for s in range(2):
            re = out[:HALF, s * ROOT : (s + 1) * ROOT]
            im = out[HALF:, s * ROOT : (s + 1) * ROOT]
            z_hi, z_lo = split(
                jnp.concatenate([re * cos_t + im * sin_t, im * cos_t - re * sin_t], axis=1)
            )
            at = row + (r + s) * HALF
            zbuf[at : at + HALF, 0 : 2 * ROOT] = z_hi
            zbuf[at : at + HALF, 2 * ROOT : 4 * ROOT] = z_lo
            zbuf[at : at + HALF, 4 * ROOT :] = z_hi
    return edge * edge


def squares(left, right):
    out = jnp.dot(left, right, preferred_element_type=jnp.float32)
    return out[:, :ROOT] * out[:, :ROOT] + out[:, ROOT:] * out[:, ROOT:]


def group_sums(lo_ref, hi_ref, right_ref, left_ref, right_on, left_on, per_dev, consts, scratch, put, put_edge):
    window_ref, first_ref, second_ref, twist_ref = consts
    buf, zbuf, ebuf, psum = scratch
    half_len = ROOT * HALF
    block = ROWS * HALF
    lane = lax.broadcasted_iota(jnp.int32, (ROWS, ROOT), 1)
    nyq = []
    for side, own, other, on in ((0, lo_ref, right_ref, right_on), (1, hi_ref, left_ref, left_on)):
        straddle = ((own, half_len), (other, 0)) if side == 0 else ((other, 0), (own, 0))
        first = stage_one(
            ((own, 0), (own, half_len)), window_ref, first_ref, twist_ref, buf, zbuf, ebuf, 0, side * 2 * ROWS
        )
        second = stage_one(
            straddle, window_ref, first_ref, twist_ref, buf, zbuf, ebuf, block, (side * 2 + 1) * ROWS
        )
        nyq.append(first + on * second)
        for r in range(ROWS):
            rows = pl.ds(r * HALF, HALF)
            both = jnp.concatenate([zbuf[rows, :], zbuf[pl.ds(block + r * HALF, HALF), :]], axis=0)
            power = squares(both, second_ref[...])
            psum[r * ROOT + side * HALF : r * ROOT + (side + 1) * HALF, :] = power[:HALF] + on * power[HALF:]
    for r in range(ROWS):
        put(r, jnp.transpose(psum[r * ROOT : (r + 1) * ROOT, :]))
    edge_power = squares(ebuf[...], second_ref[...])
    for side, on in ((0, right_on), (1, left_on)):
        at = side * 2 * ROWS
        mixed = edge_power[at : at + ROWS] + on * edge_power[at + ROWS : at + 2 * ROWS]
        put_edge(side, jnp.where(lane % (2 * per_dev) < per_dev, mixed, jnp.broadcast_to(nyq[side], (ROWS, ROOT))))


def compute_kernel(
    lo_ref, hi_ref, right_ref, left_ref, window_ref, first_ref, second_ref, twist_ref,
    sums_ref, edge_ref, buf, zbuf, ebuf, psum,
):
    me = lax.axis_index("tm")
    count = lax.axis_size("tm")
    right_on = (me < count - 1).astype(jnp.float32)
    left_on = (me > 0).astype(jnp.float32)

    def put(r, value):
        sums_ref[:, r, :] = value

    def put_edge(side, value):
        edge_ref[side] = value

    group_sums(
        lo_ref, hi_ref, right_ref, left_ref, right_on, left_on, HALF // count,
        (window_ref, first_ref, second_ref, twist_ref), (buf, zbuf, ebuf, psum), put, put_edge,
    )


def shifted(block, distance):
    count = lax.axis_size("tm")
    route = [(i - distance, i) for i in range(count) if 0 <= i - distance < count]
    return lax.ppermute(block, "tm", route)


def per_device(strain):
    chan_rows, time_width = strain.shape
    seg_len = ROOT * ROOT
    half_len = seg_len // 2
    assert time_width == seg_len and chan_rows % (2 * ROWS) == 0
    tm_count = lax.axis_size("tm")
    segments = 2 * tm_count - 1
    band = half_len // tm_count
    per_dev = HALF // tm_count
    first_all, second_all, twist, window, energy = tables(tm_count)
    pairs = chan_rows // 2
    groups = pairs // ROWS
    right = shifted(strain[:pairs, :half_len], -1)
    left = shifted(strain[pairs:, half_len:], 1)
    full = lambda shape: pl.BlockSpec(shape, lambda g: (0,) * len(shape))
    sums, edges = pl.pallas_call(
        compute_kernel,
        grid=(groups,),
        in_specs=[
            pl.BlockSpec((ROWS, seg_len), lambda g: (g, 0)),
            pl.BlockSpec((ROWS, seg_len), lambda g: (g + groups, 0)),
            pl.BlockSpec((ROWS, half_len), lambda g: (g, 0)),
            pl.BlockSpec((ROWS, half_len), lambda g: (g, 0)),
            full(window.shape), full(first_all.shape), full(second_all.shape), full(twist.shape),
        ],
        out_specs=[
            pl.BlockSpec((ROOT, ROWS, ROOT), lambda g: (0, g, 0)),
            pl.BlockSpec((2, ROWS, ROOT), lambda g: (0, g, 0)),
        ],
        out_shape=[
            jax.ShapeDtypeStruct((ROOT, pairs, ROOT), jnp.float32),
            jax.ShapeDtypeStruct((2, pairs, ROOT), jnp.float32),
        ],
        scratch_shapes=[
            pltpu.VMEM((ROWS * ROOT, ROOT), jnp.float32),
            pltpu.VMEM((2 * ROWS * HALF, 6 * ROOT), jnp.bfloat16),
            pltpu.VMEM((4 * ROWS, 6 * ROOT), jnp.bfloat16),
            pltpu.VMEM((ROWS * ROOT, ROOT), jnp.float32),
        ],
        name="periodograms",
    )(strain, strain, right, left, window, first_all, second_all, twist)
    mine = lax.psum_scatter(sums, "tm", scatter_dimension=0, tiled=True)
    edges = lax.psum(edges, "tm")
    me = lax.axis_index("tm")
    own_edges = lax.dynamic_slice_in_dim(edges, me * 2 * per_dev, per_dev, axis=2)
    front, back = mine[:per_dev], mine[per_dev:]
    halves = []
    for side in range(2):
        lanes = slice(side * HALF, (side + 1) * HALF)
        middle = jnp.transpose(own_edges[side])[:, :, None]
        mirrored = jnp.flip(back[:, :, lanes][:, :, 1:], axis=2)
        joined = jnp.concatenate([front[:, :, lanes], middle, mirrored], axis=2)
        halves.append(jnp.transpose(joined, (1, 0, 2)).reshape(pairs, band))
    band_total = jnp.concatenate(halves, axis=0)
    bin_index = me * band + jnp.arange(band, dtype=jnp.int32)
    doubling = jnp.where(bin_index == 0, 1.0, 2.0).astype(jnp.float32) / (segments * energy)
    power = band_total * doubling
    nyquist = edges[:, :, per_dev].reshape(chan_rows) / (segments * energy)
    channel_sum = lax.psum(jnp.sum(power, axis=0), "chan")
    mean_power = channel_sum / (chan_rows * lax.axis_size("chan"))
    return (power, nyquist, mean_power)


def solution(mesh):
    in_specs = (P("chan", "tm"),)
    out_specs = (P("chan", "tm"), P("chan"), P("tm"))
    return jax.shard_map(
        per_device, mesh=mesh, in_specs=in_specs, out_specs=out_specs, check_vma=False
    )
```

```python
import functools

import jax
import jax.numpy as jnp
import numpy as np
from jax import lax
from jax.experimental import pallas as pl
from jax.experimental.pallas import tpu as pltpu
from jax.sharding import PartitionSpec as P

ROOT = 128
HALF = ROOT // 2
ROWS = 8


def split_np(table):
    table = table.astype(np.float32)
    high = table.astype(jnp.bfloat16)
    low = (table - high.astype(np.float32)).astype(jnp.bfloat16)
    return high, low


@functools.cache
def tables(tm_count):
    pos = np.arange(ROOT)
    short = 2.0 * np.pi * (np.outer(pos, pos) % ROOT) / ROOT
    cos_s, sin_s = np.cos(short), np.sin(short)
    first = np.concatenate([cos_s[:HALF], -sin_s[:HALF]], axis=0)
    first_hi, first_lo = split_np(first)
    first_all = np.concatenate(
        [
            np.concatenate([first_hi, first_hi], axis=1),
            np.concatenate([first_lo, first_lo], axis=1),
        ],
        axis=0,
    )
    bands = np.arange(HALF).reshape(tm_count, HALF // tm_count)
    order = np.concatenate([bands, ROOT - 1 - bands], axis=1).reshape(-1)
    cos_o, sin_o = cos_s[:, order], sin_s[:, order]
    second = np.concatenate(
        [np.concatenate([cos_o, -sin_o], axis=1), np.concatenate([sin_o, cos_o], axis=1)], axis=0
    )
    second_hi, second_lo = split_np(second)
    second_all = np.concatenate([second_hi, second_hi, second_lo], axis=0)
    long = 2.0 * np.pi * np.outer(np.arange(HALF + ROWS), pos) / (ROOT * ROOT)
    twist = np.concatenate([np.cos(long), np.sin(long)], axis=1).astype(np.float32)
    seg_len = ROOT * ROOT
    window = 0.5 - 0.5 * np.cos(2.0 * np.pi * np.arange(seg_len) / seg_len)
    energy = float(np.sum(window * window))
    return first_all, second_all, twist, window.reshape(ROOT, ROOT).astype(np.float32), energy


def split(value):
    high = value.astype(jnp.bfloat16)
    low = (value - high.astype(jnp.float32)).astype(jnp.bfloat16)
    return high, low


def stage_one(parts, window_ref, first_ref, twist_ref, buf, zbuf, ebuf, row, erow):
    half_len = ROOT * HALF
    total = jnp.zeros((ROWS, ROOT), jnp.float32)
    for ref, offset in parts:
        total = total + jnp.sum(
            jnp.stack([ref[:, offset + ROOT * a : offset + ROOT * (a + 1)] for a in range(HALF)]), axis=0
        )
    mean = jnp.sum(total, axis=1, keepdims=True) * (1.0 / (2 * half_len))
    mean = jnp.broadcast_to(mean, (ROWS, ROOT))
    even = jnp.zeros((ROWS, ROOT), jnp.float32)
    odd = jnp.zeros((ROWS, ROOT), jnp.float32)
    for a in range(ROOT):
        ref, offset = parts[a // HALF]
        start = offset + ROOT * (a % HALF)
        tile = (ref[:, start : start + ROOT] - mean) * window_ref[a : a + 1, :]
        buf[ROWS * a : ROWS * (a + 1), :] = tile
        if a % 2 == 0:
            even = even + tile
        else:
            odd = odd + tile
    alt = even - odd
    sign = (1 - 2 * (lax.broadcasted_iota(jnp.int32, (ROWS, ROOT), 1) % 2)).astype(jnp.float32)
    edge = jnp.sum((even + odd) * sign, axis=1, keepdims=True)
    turn = twist_ref[HALF : HALF + 1, :]
    high, low = split(jnp.concatenate([alt * turn[:, :ROOT], -alt * turn[:, ROOT:]], axis=1))
    ebuf[erow : erow + ROWS, :] = jnp.concatenate([high, low, high], axis=1)
    cos_t, sin_t = twist_ref[:HALF, :ROOT], twist_ref[:HALF, ROOT:]
    for r in range(0, ROWS, 2):
        pair = jnp.concatenate(
            [buf[pl.ds(r, ROOT, stride=ROWS), :], buf[pl.ds(r + 1, ROOT, stride=ROWS), :]], axis=1
        )
        high, low = split(pair)
        out = jnp.dot(
            first_ref[...], jnp.concatenate([high, low], axis=0), preferred_element_type=jnp.float32
        )
        out = out[:ROOT] + out[ROOT:]
        for s in range(2):
            re = out[:HALF, s * ROOT : (s + 1) * ROOT]
            im = out[HALF:, s * ROOT : (s + 1) * ROOT]
            z_hi, z_lo = split(
                jnp.concatenate([re * cos_t + im * sin_t, im * cos_t - re * sin_t], axis=1)
            )
            at = row + (r + s) * HALF
            zbuf[at : at + HALF, 0 : 2 * ROOT] = z_hi
            zbuf[at : at + HALF, 2 * ROOT : 4 * ROOT] = z_lo
            zbuf[at : at + HALF, 4 * ROOT :] = z_hi
    return edge * edge


def squares(left, right):
    out = jnp.dot(left, right, preferred_element_type=jnp.float32)
    return out[:, :ROOT] * out[:, :ROOT] + out[:, ROOT:] * out[:, ROOT:]


def group_sums(lo_ref, hi_ref, right_ref, left_ref, right_on, left_on, per_dev, consts, scratch, put, put_edge):
    window_ref, first_ref, second_ref, twist_ref = consts
    buf, zbuf, ebuf, psum = scratch
    half_len = ROOT * HALF
    block = ROWS * HALF
    lane = lax.broadcasted_iota(jnp.int32, (ROWS, ROOT), 1)
    nyq = []
    for side, own, other, on in ((0, lo_ref, right_ref, right_on), (1, hi_ref, left_ref, left_on)):
        straddle = ((own, half_len), (other, 0)) if side == 0 else ((other, 0), (own, 0))
        first = stage_one(
            ((own, 0), (own, half_len)), window_ref, first_ref, twist_ref, buf, zbuf, ebuf, 0, side * 2 * ROWS
        )
        second = stage_one(
            straddle, window_ref, first_ref, twist_ref, buf, zbuf, ebuf, block, (side * 2 + 1) * ROWS
        )
        nyq.append(first + on * second)
        for r in range(ROWS):
            rows = pl.ds(r * HALF, HALF)
            both = jnp.concatenate([zbuf[rows, :], zbuf[pl.ds(block + r * HALF, HALF), :]], axis=0)
            power = squares(both, second_ref[...])
            psum[r * ROOT + side * HALF : r * ROOT + (side + 1) * HALF, :] = power[:HALF] + on * power[HALF:]
    for r in range(ROWS):
        put(r, jnp.transpose(psum[r * ROOT : (r + 1) * ROOT, :]))
    edge_power = squares(ebuf[...], second_ref[...])
    for side, on in ((0, right_on), (1, left_on)):
        at = side * 2 * ROWS
        mixed = edge_power[at : at + ROWS] + on * edge_power[at + ROWS : at + 2 * ROWS]
        put_edge(side, jnp.where(lane % (2 * per_dev) < per_dev, mixed, jnp.broadcast_to(nyq[side], (ROWS, ROOT))))


def welch_kernel(
    pieces, strain_ref, window_ref, first_ref, second_ref, twist_ref, mine_ref, edge_out_ref,
    data, right_half, left_half, sums, edge_rows, edge_sums, from_left, from_right, edge_left, edge_right,
    buf, zbuf, ebuf, psum,
    load_sem, halo_send, halo_recv, line_send, line_recv, edge_send, edge_recv,
):
    me = lax.axis_index("tm")
    count = lax.axis_size("tm")
    per_dev = HALF // count
    rows = 2 * per_dev
    half_len = ROOT * HALF
    pairs = sums.shape[1]
    groups = pairs // ROWS
    width = pairs // pieces
    has_left, has_right = me > 0, me < count - 1
    right_on, left_on = has_right.astype(jnp.float32), has_left.astype(jnp.float32)

    def block(g, side):
        return pl.ds(pl.multiple_of(side * pairs + g * ROWS, ROWS), ROWS)

    def load(g, side):
        return pltpu.make_async_copy(
            strain_ref.at[block(g, side)], data.at[block(g, side)], load_sem.at[side, g]
        )

    def halo(g, side):
        source = strain_ref.at[block(g, side), pl.ds(side * half_len, half_len)]
        target = (right_half, left_half)[side]
        return pltpu.make_async_remote_copy(
            src_ref=source, dst_ref=target.at[block(g, 0)],
            send_sem=halo_send.at[side, g], recv_sem=halo_recv.at[side, g],
            device_id={"tm": me + (1 if side else -1)}, device_id_type=pl.DeviceIdType.MESH,
        )

    @pl.loop(0, groups)
    def _(g):
        load(g, 0).start()
        load(g, 1).start()

    barrier = pltpu.get_barrier_semaphore()
    for exists, step in ((has_left, -1), (has_right, 1)):
        @pl.when(exists)
        def _():
            pl.semaphore_signal(
                barrier, inc=1, device_id={"tm": me + step}, device_id_type=pl.DeviceIdType.MESH
            )
    pl.semaphore_wait(barrier, has_left.astype(jnp.int32) + has_right.astype(jnp.int32))

    @pl.loop(0, groups)
    def _(g):
        for side, exists in ((0, has_left), (1, has_right)):
            @pl.when(exists)
            def _():
                halo(g, side).start()

    edge_rows[...] = jnp.zeros_like(edge_rows)
    for side, exists, ref in ((0, has_right, right_half), (1, has_left, left_half)):
        @pl.when(jnp.logical_not(exists))
        def _():
            ref[...] = jnp.zeros_like(ref)

    @pl.loop(0, groups)
    def _(g):
        load(g, 0).wait()
        load(g, 1).wait()
        for side, exists in ((0, has_right), (1, has_left)):
            @pl.when(exists)
            def _():
                halo(g, side).wait_recv()

        def put(r, value):
            sums[:, g * ROWS + r, :] = value

        def put_edge(side, value):
            edge_rows[block(g, side), :] = value

        group_sums(
            data.at[block(g, 0)], data.at[block(g, 1)], right_half.at[block(g, 0)], left_half.at[block(g, 0)],
            right_on, left_on, per_dev,
            (window_ref, first_ref, second_ref, twist_ref), (buf, zbuf, ebuf, psum), put, put_edge,
        )

    spread = edge_sums.shape[1]
    for s in range(spread):
        edge_sums[:, s, :] = jnp.transpose(edge_rows[s * ROOT : (s + 1) * ROOT, :])

    def chunk_of(m, side):
        far = m // pieces
        return far if side else count - 1 - far

    def sum_part(m, side):
        q = lax.rem(m, pieces)
        return sums.at[pl.ds(chunk_of(m, side) * rows, rows), pl.ds(pl.multiple_of(q * width, ROWS), width)]

    def edge_part(m, side):
        return edge_sums.at[pl.ds(chunk_of(m, side) * rows, rows)]

    def line(m, side):
        target = (from_left, from_right)[side]
        return pltpu.make_async_remote_copy(
            src_ref=sum_part(m, side), dst_ref=target.at[m],
            send_sem=line_send.at[side, m], recv_sem=line_recv.at[side, m],
            device_id={"tm": me + (-1 if side else 1)}, device_id_type=pl.DeviceIdType.MESH,
        )

    def edge_line(m, side):
        target = (edge_left, edge_right)[side]
        far = m // pieces
        return pltpu.make_async_remote_copy(
            src_ref=edge_part(m, side), dst_ref=target.at[far],
            send_sem=edge_send.at[side, far], recv_sem=edge_recv.at[side, far],
            device_id={"tm": me + (-1 if side else 1)}, device_id_type=pl.DeviceIdType.MESH,
        )

    def take(m, side):
        line(m, side).wait_recv()
        part = sum_part(m, side)
        part[...] = part[...] + (from_left, from_right)[side][m]

        @pl.when(lax.rem(m, pieces) == 0)
        def _():
            edge_line(m, side).wait_recv()
            edge = edge_part(m, side)
            edge[...] = edge[...] + (edge_left, edge_right)[side][m // pieces]

    messages = (count - 1) * pieces

    @pl.loop(0, messages + count - 1)
    def _(t):
        for side in range(2):
            place = count - 1 - me if side else me
            m = t - place

            @pl.when(jnp.logical_and(m >= 0, m < (count - 1 - place) * pieces))
            def _():
                @pl.when(place > 0)
                def _():
                    take(m, side)

                line(m, side).start()

                @pl.when(lax.rem(m, pieces) == 0)
                def _():
                    edge_line(m, side).start()

    for side in range(2):
        place = count - 1 - me if side else me

        @pl.when(place > 0)
        def _():
            @pl.loop(0, pieces)
            def _(q):
                take((count - 1 - place) * pieces + q, side)

    mine_ref[...] = sums[pl.ds(me * rows, rows)]
    edge_out_ref[...] = edge_sums[pl.ds(me * rows, rows)]

    @pl.loop(0, groups)
    def _(g):
        for side, exists in ((0, has_left), (1, has_right)):
            @pl.when(exists)
            def _():
                halo(g, side).wait_send()

    @pl.loop(0, messages)
    def _(m):
        for side in range(2):
            place = count - 1 - me if side else me

            @pl.when(m < (count - 1 - place) * pieces)
            def _():
                line(m, side).wait_send()

                @pl.when(lax.rem(m, pieces) == 0)
                def _():
                    edge_line(m, side).wait_send()


def per_device(strain):
    chan_rows, time_width = strain.shape
    seg_len = ROOT * ROOT
    half_len = seg_len // 2
    assert time_width == seg_len and chan_rows % (2 * ROWS) == 0
    tm_count = lax.axis_size("tm")
    segments = 2 * tm_count - 1
    band = half_len // tm_count
    per_dev = HALF // tm_count
    rows = 2 * per_dev
    first_all, second_all, twist, window, energy = tables(tm_count)
    pairs = chan_rows // 2
    groups = pairs // ROWS
    pieces = 4 if groups % 4 == 0 else 1
    spread = -(-chan_rows // ROOT)
    messages = (tm_count - 1) * pieces
    vmem = pl.BlockSpec(memory_space=pltpu.VMEM)
    f32 = jnp.float32
    mine, own_edges = pl.pallas_call(
        functools.partial(welch_kernel, pieces),
        in_specs=[pl.BlockSpec(memory_space=pl.ANY)] + [vmem] * 4,
        out_specs=[vmem, vmem],
        out_shape=[
            jax.ShapeDtypeStruct((rows, pairs, ROOT), f32),
            jax.ShapeDtypeStruct((rows, spread, ROOT), f32),
        ],
        scratch_shapes=[
            pltpu.VMEM((chan_rows, seg_len), f32),
            pltpu.VMEM((pairs, half_len), f32),
            pltpu.VMEM((pairs, half_len), f32),
            pltpu.VMEM((ROOT, pairs, ROOT), f32),
            pltpu.VMEM((spread * ROOT, ROOT), f32),
            pltpu.VMEM((ROOT, spread, ROOT), f32),
            pltpu.VMEM((messages, rows, pairs // pieces, ROOT), f32),
            pltpu.VMEM((messages, rows, pairs // pieces, ROOT), f32),
            pltpu.VMEM((tm_count - 1, rows, spread, ROOT), f32),
            pltpu.VMEM((tm_count - 1, rows, spread, ROOT), f32),
            pltpu.VMEM((ROWS * ROOT, ROOT), f32),
            pltpu.VMEM((2 * ROWS * HALF, 6 * ROOT), jnp.bfloat16),
            pltpu.VMEM((4 * ROWS, 6 * ROOT), jnp.bfloat16),
            pltpu.VMEM((ROWS * ROOT, ROOT), f32),
            pltpu.SemaphoreType.DMA((2, groups)),
            pltpu.SemaphoreType.DMA((2, groups)),
            pltpu.SemaphoreType.DMA((2, groups)),
            pltpu.SemaphoreType.DMA((2, messages)),
            pltpu.SemaphoreType.DMA((2, messages)),
            pltpu.SemaphoreType.DMA((2, tm_count - 1)),
            pltpu.SemaphoreType.DMA((2, tm_count - 1)),
        ],
        compiler_params=pltpu.CompilerParams(
            collective_id=0, has_side_effects=True, vmem_limit_bytes=60 * 2**20
        ),
        name="welch",
    )(strain, window, first_all, second_all, twist)
    me = lax.axis_index("tm")
    front, back = mine[:per_dev], mine[per_dev:]
    middle = own_edges[:per_dev].reshape(per_dev, -1)[:, :chan_rows]
    halves = []
    for side in range(2):
        lanes = slice(side * HALF, (side + 1) * HALF)
        mirrored = jnp.flip(back[:, :, lanes][:, :, 1:], axis=2)
        centre = middle[:, side * pairs : (side + 1) * pairs, None]
        joined = jnp.concatenate([front[:, :, lanes], centre, mirrored], axis=2)
        halves.append(jnp.transpose(joined, (1, 0, 2)).reshape(pairs, band))
    band_total = jnp.concatenate(halves, axis=0)
    bin_index = me * band + jnp.arange(band, dtype=jnp.int32)
    doubling = jnp.where(bin_index == 0, 1.0, 2.0).astype(jnp.float32) / (segments * energy)
    power = band_total * doubling
    nyquist = own_edges[per_dev].reshape(-1)[:chan_rows] / (segments * energy)
    channel_sum = lax.psum(jnp.sum(power, axis=0), "chan")
    mean_power = channel_sum / (chan_rows * lax.axis_size("chan"))
    return (power, nyquist, mean_power)


def solution(mesh):
    in_specs = (P("chan", "tm"),)
    out_specs = (P("chan", "tm"), P("chan"), P("tm"))
    return jax.shard_map(
        per_device, mesh=mesh, in_specs=in_specs, out_specs=out_specs, check_vma=False
    )
```

```python
import functools

import jax
import jax.numpy as jnp
import numpy as np
from jax import lax
from jax.experimental import pallas as pl
from jax.experimental.pallas import tpu as pltpu
from jax.sharding import PartitionSpec as P

ROOT = 128
HALF = ROOT // 2
ROWS = 8


def split_np(table):
    table = table.astype(np.float32)
    high = table.astype(jnp.bfloat16)
    low = (table - high.astype(np.float32)).astype(jnp.bfloat16)
    return high, low


@functools.cache
def tables(tm_count):
    pos = np.arange(ROOT)
    short = 2.0 * np.pi * (np.outer(pos, pos) % ROOT) / ROOT
    cos_s, sin_s = np.cos(short), np.sin(short)
    first = np.concatenate([cos_s[:HALF], -sin_s[:HALF]], axis=0)
    first_hi, first_lo = split_np(first)
    first_all = np.concatenate(
        [
            np.concatenate([first_hi, first_hi], axis=1),
            np.concatenate([first_lo, first_lo], axis=1),
        ],
        axis=0,
    )
    bands = np.arange(HALF).reshape(tm_count, HALF // tm_count)
    order = np.concatenate([bands, ROOT - 1 - bands], axis=1).reshape(-1)
    cos_o, sin_o = cos_s[:, order], sin_s[:, order]
    second = np.concatenate(
        [np.concatenate([cos_o, -sin_o], axis=1), np.concatenate([sin_o, cos_o], axis=1)], axis=0
    )
    second_hi, second_lo = split_np(second)
    second_all = np.concatenate([second_hi, second_hi, second_lo], axis=0)
    long = 2.0 * np.pi * np.outer(np.arange(HALF + ROWS), pos) / (ROOT * ROOT)
    twist = np.concatenate([np.cos(long), np.sin(long)], axis=1).astype(np.float32)
    mirror = np.zeros((2 * ROOT, 2 * ROOT), np.float32)
    for side in range(2):
        for k in range(HALF):
            mirror[side * HALF + k, side * ROOT + k] = 1.0
            if k > 0:
                mirror[ROOT + side * HALF + k, side * ROOT + ROOT - k] = 1.0
    seg_len = ROOT * ROOT
    window = 0.5 - 0.5 * np.cos(2.0 * np.pi * np.arange(seg_len) / seg_len)
    energy = float(np.sum(window * window))
    return first_all, second_all, twist, window.reshape(ROOT, ROOT).astype(np.float32), mirror, energy


def split(value):
    high = value.astype(jnp.bfloat16)
    low = (value - high.astype(jnp.float32)).astype(jnp.bfloat16)
    return high, low


def stage_one(parts, window_ref, first_ref, twist_ref, buf, zbuf, ebuf, row, erow):
    half_len = ROOT * HALF
    total = jnp.zeros((ROWS, ROOT), jnp.float32)
    for ref, offset in parts:
        total = total + jnp.sum(
            jnp.stack([ref[:, offset + ROOT * a : offset + ROOT * (a + 1)] for a in range(HALF)]), axis=0
        )
    mean = jnp.sum(total, axis=1, keepdims=True) * (1.0 / (2 * half_len))
    mean = jnp.broadcast_to(mean, (ROWS, ROOT))
    even = jnp.zeros((ROWS, ROOT), jnp.float32)
    odd = jnp.zeros((ROWS, ROOT), jnp.float32)
    for a in range(ROOT):
        ref, offset = parts[a // HALF]
        start = offset + ROOT * (a % HALF)
        tile = (ref[:, start : start + ROOT] - mean) * window_ref[a : a + 1, :]
        buf[ROWS * a : ROWS * (a + 1), :] = tile
        if a % 2 == 0:
            even = even + tile
        else:
            odd = odd + tile
    alt = even - odd
    sign = (1 - 2 * (lax.broadcasted_iota(jnp.int32, (ROWS, ROOT), 1) % 2)).astype(jnp.float32)
    edge = jnp.sum((even + odd) * sign, axis=1, keepdims=True)
    turn = twist_ref[HALF : HALF + 1, :]
    high, low = split(jnp.concatenate([alt * turn[:, :ROOT], -alt * turn[:, ROOT:]], axis=1))
    ebuf[erow : erow + ROWS, :] = jnp.concatenate([high, low, high], axis=1)
    cos_t, sin_t = twist_ref[:HALF, :ROOT], twist_ref[:HALF, ROOT:]
    for r in range(0, ROWS, 2):
        pair = jnp.concatenate(
            [buf[pl.ds(r, ROOT, stride=ROWS), :], buf[pl.ds(r + 1, ROOT, stride=ROWS), :]], axis=1
        )
        high, low = split(pair)
        out = jnp.dot(
            first_ref[...], jnp.concatenate([high, low], axis=0), preferred_element_type=jnp.float32
        )
        out = out[:ROOT] + out[ROOT:]
        for s in range(2):
            re = out[:HALF, s * ROOT : (s + 1) * ROOT]
            im = out[HALF:, s * ROOT : (s + 1) * ROOT]
            z_hi, z_lo = split(
                jnp.concatenate([re * cos_t + im * sin_t, im * cos_t - re * sin_t], axis=1)
            )
            at = row + (r + s) * HALF
            zbuf[at : at + HALF, 0 : 2 * ROOT] = z_hi
            zbuf[at : at + HALF, 2 * ROOT : 4 * ROOT] = z_lo
            zbuf[at : at + HALF, 4 * ROOT :] = z_hi
    return edge * edge


def squares(left, right):
    out = jnp.dot(left, right, preferred_element_type=jnp.float32)
    return out[:, :ROOT] * out[:, :ROOT] + out[:, ROOT:] * out[:, ROOT:]


def group_sums(lo_ref, hi_ref, right_ref, left_ref, right_on, left_on, per_dev, consts, scratch, put, put_edge):
    window_ref, first_ref, second_ref, twist_ref = consts
    buf, zbuf, ebuf, psum = scratch
    half_len = ROOT * HALF
    block = ROWS * HALF
    lane = lax.broadcasted_iota(jnp.int32, (ROWS, ROOT), 1)
    nyq = []
    for side, own, other, on in ((0, lo_ref, right_ref, right_on), (1, hi_ref, left_ref, left_on)):
        straddle = ((own, half_len), (other, 0)) if side == 0 else ((other, 0), (own, 0))
        first = stage_one(
            ((own, 0), (own, half_len)), window_ref, first_ref, twist_ref, buf, zbuf, ebuf, 0, side * 2 * ROWS
        )
        second = stage_one(
            straddle, window_ref, first_ref, twist_ref, buf, zbuf, ebuf, block, (side * 2 + 1) * ROWS
        )
        nyq.append(first + on * second)
        for r in range(ROWS):
            rows = pl.ds(r * HALF, HALF)
            both = jnp.concatenate([zbuf[rows, :], zbuf[pl.ds(block + r * HALF, HALF), :]], axis=0)
            power = squares(both, second_ref[...])
            psum[r * ROOT + side * HALF : r * ROOT + (side + 1) * HALF, :] = power[:HALF] + on * power[HALF:]
    for r in range(ROWS):
        put(r, jnp.transpose(psum[r * ROOT : (r + 1) * ROOT, :]))
    edge_power = squares(ebuf[...], second_ref[...])
    for side, on in ((0, right_on), (1, left_on)):
        at = side * 2 * ROWS
        mixed = edge_power[at : at + ROWS] + on * edge_power[at + ROWS : at + 2 * ROWS]
        put_edge(side, jnp.where(lane % (2 * per_dev) < per_dev, mixed, jnp.broadcast_to(nyq[side], (ROWS, ROOT))))


def welch_kernel(
    pieces, scale, strain_ref, window_ref, first_ref, second_ref, twist_ref, mirror_ref,
    power_ref, nyquist_ref, mean_ref,
    data, right_half, left_half, sums, edge_rows, edge_sums, from_left, from_right, edge_left, edge_right,
    buf, zbuf, ebuf, psum, channel_sums, channel_from,
    load_sem, halo_send, halo_recv, line_send, line_recv, edge_send, edge_recv, chan_send, chan_recv,
):
    chan, chan_count = lax.axis_index("chan"), lax.axis_size("chan")
    me = lax.axis_index("tm")
    count = lax.axis_size("tm")
    per_dev = HALF // count
    rows = 2 * per_dev
    half_len = ROOT * HALF
    pairs = sums.shape[1]
    groups = pairs // ROWS
    width = pairs // pieces
    has_left, has_right = me > 0, me < count - 1
    right_on, left_on = has_right.astype(jnp.float32), has_left.astype(jnp.float32)

    def block(g, side):
        return pl.ds(pl.multiple_of(side * pairs + g * ROWS, ROWS), ROWS)

    def load(g, side):
        return pltpu.make_async_copy(
            strain_ref.at[block(g, side)], data.at[block(g, side)], load_sem.at[side, g]
        )

    def halo(g, side):
        source = strain_ref.at[block(g, side), pl.ds(side * half_len, half_len)]
        target = (right_half, left_half)[side]
        return pltpu.make_async_remote_copy(
            src_ref=source, dst_ref=target.at[block(g, 0)],
            send_sem=halo_send.at[side, g], recv_sem=halo_recv.at[side, g],
            device_id={"tm": me + (1 if side else -1)}, device_id_type=pl.DeviceIdType.MESH,
        )

    @pl.loop(0, groups)
    def _(g):
        load(g, 0).start()
        load(g, 1).start()

    barrier = pltpu.get_barrier_semaphore()
    for exists, step in ((has_left, -1), (has_right, 1)):
        @pl.when(exists)
        def _():
            pl.semaphore_signal(
                barrier, inc=1, device_id={"tm": me + step}, device_id_type=pl.DeviceIdType.MESH
            )
    for k in range(1, chan_count):
        pl.semaphore_signal(
            barrier, inc=1, device_id={"chan": lax.rem(chan + k, chan_count)},
            device_id_type=pl.DeviceIdType.MESH,
        )
    pl.semaphore_wait(
        barrier, has_left.astype(jnp.int32) + has_right.astype(jnp.int32) + (chan_count - 1)
    )

    @pl.loop(0, groups)
    def _(g):
        for side, exists in ((0, has_left), (1, has_right)):
            @pl.when(exists)
            def _():
                halo(g, side).start()

    edge_rows[...] = jnp.zeros_like(edge_rows)
    for side, exists, ref in ((0, has_right, right_half), (1, has_left, left_half)):
        @pl.when(jnp.logical_not(exists))
        def _():
            ref[...] = jnp.zeros_like(ref)

    @pl.loop(0, groups)
    def _(g):
        load(g, 0).wait()
        load(g, 1).wait()
        for side, exists in ((0, has_right), (1, has_left)):
            @pl.when(exists)
            def _():
                halo(g, side).wait_recv()

        def put(r, value):
            sums[:, g * ROWS + r, :] = value

        def put_edge(side, value):
            edge_rows[block(g, side), :] = value

        group_sums(
            data.at[block(g, 0)], data.at[block(g, 1)], right_half.at[block(g, 0)], left_half.at[block(g, 0)],
            right_on, left_on, per_dev,
            (window_ref, first_ref, second_ref, twist_ref), (buf, zbuf, ebuf, psum), put, put_edge,
        )

    spread = edge_sums.shape[1]
    for s in range(spread):
        edge_sums[:, s, :] = jnp.transpose(edge_rows[s * ROOT : (s + 1) * ROOT, :])

    def chunk_of(m, side):
        far = m // pieces
        return far if side else count - 1 - far

    def sum_part(m, side):
        q = lax.rem(m, pieces)
        return sums.at[pl.ds(chunk_of(m, side) * rows, rows), pl.ds(pl.multiple_of(q * width, ROWS), width)]

    def edge_part(m, side):
        return edge_sums.at[pl.ds(chunk_of(m, side) * rows, rows)]

    def line(m, side):
        target = (from_left, from_right)[side]
        return pltpu.make_async_remote_copy(
            src_ref=sum_part(m, side), dst_ref=target.at[m],
            send_sem=line_send.at[side, m], recv_sem=line_recv.at[side, m],
            device_id={"tm": me + (-1 if side else 1)}, device_id_type=pl.DeviceIdType.MESH,
        )

    def edge_line(m, side):
        target = (edge_left, edge_right)[side]
        far = m // pieces
        return pltpu.make_async_remote_copy(
            src_ref=edge_part(m, side), dst_ref=target.at[far],
            send_sem=edge_send.at[side, far], recv_sem=edge_recv.at[side, far],
            device_id={"tm": me + (-1 if side else 1)}, device_id_type=pl.DeviceIdType.MESH,
        )

    def take(m, side):
        line(m, side).wait_recv()
        part = sum_part(m, side)
        part[...] = part[...] + (from_left, from_right)[side][m]

        @pl.when(lax.rem(m, pieces) == 0)
        def _():
            edge_line(m, side).wait_recv()
            edge = edge_part(m, side)
            edge[...] = edge[...] + (edge_left, edge_right)[side][m // pieces]

    messages = (count - 1) * pieces

    @pl.loop(0, messages + count - 1)
    def _(t):
        for side in range(2):
            place = count - 1 - me if side else me
            m = t - place

            @pl.when(jnp.logical_and(m >= 0, m < (count - 1 - place) * pieces))
            def _():
                @pl.when(place > 0)
                def _():
                    take(m, side)

                line(m, side).start()

                @pl.when(lax.rem(m, pieces) == 0)
                def _():
                    edge_line(m, side).start()

    for side in range(2):
        place = count - 1 - me if side else me

        @pl.when(place > 0)
        def _():
            @pl.loop(0, pieces)
            def _(q):
                take((count - 1 - place) * pieces + q, side)

    nyquist_ref[...] = edge_sums[me * rows + per_dev] * scale
    for s in range(spread):
        strip = jnp.concatenate(
            [edge_sums[me * rows + j, s : s + 1, :] for j in range(per_dev)]
            + [jnp.zeros((ROOT - per_dev, ROOT), jnp.float32)],
            axis=0,
        )
        edge_rows[s * ROOT : (s + 1) * ROOT, :] = jnp.transpose(strip)
    lanes = lax.broadcasted_iota(jnp.int32, (1, ROOT), 1)
    for j in range(per_dev):
        both = jnp.concatenate([sums[me * rows + j], sums[me * rows + per_dev + j]], axis=1)
        placed = jnp.dot(
            both, mirror_ref[...], precision=lax.Precision.HIGHEST, preferred_element_type=jnp.float32
        )
        factor = jnp.where(jnp.logical_and(lanes == 0, me + j == 0), scale, 2.0 * scale)
        column = jnp.zeros((1, ROOT), jnp.float32)
        for side in range(2):
            middle = edge_rows[side * pairs : (side + 1) * pairs, j : j + 1]
            value = jnp.where(lanes == HALF, middle, placed[:, side * ROOT : (side + 1) * ROOT]) * factor
            power_ref[side * pairs : (side + 1) * pairs, j * ROOT : (j + 1) * ROOT] = value
            column = column + jnp.sum(value, axis=0, keepdims=True)
        channel_sums[j : j + 1, :] = column

    def chan_copy(k):
        return pltpu.make_async_remote_copy(
            src_ref=channel_sums, dst_ref=channel_from.at[k],
            send_sem=chan_send.at[k], recv_sem=chan_recv.at[k],
            device_id={"chan": lax.rem(chan + k, chan_count)}, device_id_type=pl.DeviceIdType.MESH,
        )

    for k in range(1, chan_count):
        chan_copy(k).start()

    @pl.loop(0, groups)
    def _(g):
        for side, exists in ((0, has_left), (1, has_right)):
            @pl.when(exists)
            def _():
                halo(g, side).wait_send()

    @pl.loop(0, messages)
    def _(m):
        for side in range(2):
            place = count - 1 - me if side else me

            @pl.when(m < (count - 1 - place) * pieces)
            def _():
                line(m, side).wait_send()

                @pl.when(lax.rem(m, pieces) == 0)
                def _():
                    edge_line(m, side).wait_send()

    channel_from[0] = channel_sums[...]
    for k in range(1, chan_count):
        chan_copy(k).wait()
    total = jnp.zeros_like(channel_sums)
    for source in range(chan_count):
        total = total + channel_from[lax.rem(chan - source + chan_count, chan_count)]
    mean_ref[...] = total * (1.0 / (2 * pairs * chan_count))


def per_device(strain):
    chan_rows, time_width = strain.shape
    seg_len = ROOT * ROOT
    half_len = seg_len // 2
    assert time_width == seg_len and chan_rows % (2 * ROWS) == 0
    tm_count = lax.axis_size("tm")
    segments = 2 * tm_count - 1
    band = half_len // tm_count
    per_dev = HALF // tm_count
    rows = 2 * per_dev
    first_all, second_all, twist, window, mirror, energy = tables(tm_count)
    pairs = chan_rows // 2
    groups = pairs // ROWS
    pieces = 4 if groups % 4 == 0 else 1
    spread = -(-chan_rows // ROOT)
    messages = (tm_count - 1) * pieces
    vmem = pl.BlockSpec(memory_space=pltpu.VMEM)
    f32 = jnp.float32
    power, nyquist, mean_power = pl.pallas_call(
        functools.partial(welch_kernel, pieces, 1.0 / (segments * energy)),
        in_specs=[pl.BlockSpec(memory_space=pl.ANY)] + [vmem] * 5,
        out_specs=[vmem] * 3,
        out_shape=[
            jax.ShapeDtypeStruct((chan_rows, band), f32),
            jax.ShapeDtypeStruct((spread, ROOT), f32),
            jax.ShapeDtypeStruct((per_dev, ROOT), f32),
        ],
        scratch_shapes=[
            pltpu.VMEM((chan_rows, seg_len), f32),
            pltpu.VMEM((pairs, half_len), f32),
            pltpu.VMEM((pairs, half_len), f32),
            pltpu.VMEM((ROOT, pairs, ROOT), f32),
            pltpu.VMEM((spread * ROOT, ROOT), f32),
            pltpu.VMEM((ROOT, spread, ROOT), f32),
            pltpu.VMEM((messages, rows, pairs // pieces, ROOT), f32),
            pltpu.VMEM((messages, rows, pairs // pieces, ROOT), f32),
            pltpu.VMEM((tm_count - 1, rows, spread, ROOT), f32),
            pltpu.VMEM((tm_count - 1, rows, spread, ROOT), f32),
            pltpu.VMEM((ROWS * ROOT, ROOT), f32),
            pltpu.VMEM((2 * ROWS * HALF, 6 * ROOT), jnp.bfloat16),
            pltpu.VMEM((4 * ROWS, 6 * ROOT), jnp.bfloat16),
            pltpu.VMEM((ROWS * ROOT, ROOT), f32),
            pltpu.VMEM((per_dev, ROOT), f32),
            pltpu.VMEM((lax.axis_size("chan"), per_dev, ROOT), f32),
            pltpu.SemaphoreType.DMA((2, groups)),
            pltpu.SemaphoreType.DMA((2, groups)),
            pltpu.SemaphoreType.DMA((2, groups)),
            pltpu.SemaphoreType.DMA((2, messages)),
            pltpu.SemaphoreType.DMA((2, messages)),
            pltpu.SemaphoreType.DMA((2, tm_count - 1)),
            pltpu.SemaphoreType.DMA((2, tm_count - 1)),
            pltpu.SemaphoreType.DMA((lax.axis_size("chan"),)),
            pltpu.SemaphoreType.DMA((lax.axis_size("chan"),)),
        ],
        compiler_params=pltpu.CompilerParams(
            collective_id=0, has_side_effects=True, vmem_limit_bytes=60 * 2**20
        ),
        name="welch",
    )(strain, window, first_all, second_all, twist, mirror)
    return (power, nyquist.reshape(-1)[:chan_rows], mean_power.reshape(-1))


def solution(mesh):
    in_specs = (P("chan", "tm"),)
    out_specs = (P("chan", "tm"), P("chan"), P("tm"))
    return jax.shard_map(
        per_device, mesh=mesh, in_specs=in_specs, out_specs=out_specs, check_vma=False
    )
```

```python
import functools

import jax
import jax.numpy as jnp
import numpy as np
from jax import lax
from jax.experimental import pallas as pl
from jax.experimental.pallas import tpu as pltpu
from jax.sharding import PartitionSpec as P

ROOT = 128
HALF = ROOT // 2
ROWS = 8


def split_np(table):
    table = table.astype(np.float32)
    high = table.astype(jnp.bfloat16)
    low = (table - high.astype(np.float32)).astype(jnp.bfloat16)
    return high, low


@functools.cache
def tables(tm_count):
    pos = np.arange(ROOT)
    short = 2.0 * np.pi * (np.outer(pos, pos) % ROOT) / ROOT
    cos_s, sin_s = np.cos(short), np.sin(short)
    first = np.concatenate([cos_s[:HALF], -sin_s[:HALF]], axis=0)
    first_hi, first_lo = split_np(first)
    first_all = np.concatenate(
        [
            np.concatenate([first_hi, first_hi], axis=1),
            np.concatenate([first_lo, first_lo], axis=1),
        ],
        axis=0,
    )
    bands = np.arange(HALF).reshape(tm_count, HALF // tm_count)
    order = np.concatenate([bands, ROOT - 1 - bands], axis=1).reshape(-1)
    cos_o, sin_o = cos_s[:, order], sin_s[:, order]
    second = np.concatenate(
        [np.concatenate([cos_o, -sin_o], axis=1), np.concatenate([sin_o, cos_o], axis=1)], axis=0
    )
    second_hi, second_lo = split_np(second)
    second_all = np.concatenate([second_hi, second_hi, second_lo], axis=0)
    long = 2.0 * np.pi * np.outer(np.arange(HALF + ROWS), pos) / (ROOT * ROOT)
    twist = np.concatenate([np.cos(long), np.sin(long)], axis=1).astype(np.float32)
    mirror = np.zeros((2 * ROOT, 2 * ROOT), np.float32)
    for side in range(2):
        for k in range(HALF):
            mirror[side * HALF + k, side * ROOT + k] = 1.0
            if k > 0:
                mirror[ROOT + side * HALF + k, side * ROOT + ROOT - k] = 1.0
    seg_len = ROOT * ROOT
    window = 0.5 - 0.5 * np.cos(2.0 * np.pi * np.arange(seg_len) / seg_len)
    energy = float(np.sum(window * window))
    return first_all, second_all, twist, window.reshape(ROOT, ROOT).astype(np.float32), mirror, energy


def split(value):
    high = value.astype(jnp.bfloat16)
    low = (value - high.astype(jnp.float32)).astype(jnp.bfloat16)
    return high, low


def stage_one(parts, window_ref, first_ref, twist_ref, buf, zbuf, ebuf, row, erow):
    half_len = ROOT * HALF
    total = jnp.zeros((ROWS, ROOT), jnp.float32)
    for ref, offset in parts:
        total = total + jnp.sum(
            jnp.stack([ref[:, offset + ROOT * a : offset + ROOT * (a + 1)] for a in range(HALF)]), axis=0
        )
    mean = jnp.sum(total, axis=1, keepdims=True) * (1.0 / (2 * half_len))
    mean = jnp.broadcast_to(mean, (ROWS, ROOT))
    even = jnp.zeros((ROWS, ROOT), jnp.float32)
    odd = jnp.zeros((ROWS, ROOT), jnp.float32)
    for a in range(ROOT):
        ref, offset = parts[a // HALF]
        start = offset + ROOT * (a % HALF)
        tile = (ref[:, start : start + ROOT] - mean) * window_ref[a : a + 1, :]
        buf[ROWS * a : ROWS * (a + 1), :] = tile
        if a % 2 == 0:
            even = even + tile
        else:
            odd = odd + tile
    alt = even - odd
    sign = (1 - 2 * (lax.broadcasted_iota(jnp.int32, (ROWS, ROOT), 1) % 2)).astype(jnp.float32)
    edge = jnp.sum((even + odd) * sign, axis=1, keepdims=True)
    turn = twist_ref[HALF : HALF + 1, :]
    high, low = split(jnp.concatenate([alt * turn[:, :ROOT], -alt * turn[:, ROOT:]], axis=1))
    ebuf[erow : erow + ROWS, :] = jnp.concatenate([high, low, high], axis=1)
    cos_t, sin_t = twist_ref[:HALF, :ROOT], twist_ref[:HALF, ROOT:]
    for r in range(0, ROWS, 2):
        pair = jnp.concatenate(
            [buf[pl.ds(r, ROOT, stride=ROWS), :], buf[pl.ds(r + 1, ROOT, stride=ROWS), :]], axis=1
        )
        high, low = split(pair)
        out = jnp.dot(
            first_ref[...], jnp.concatenate([high, low], axis=0), preferred_element_type=jnp.float32
        )
        out = out[:ROOT] + out[ROOT:]
        for s in range(2):
            re = out[:HALF, s * ROOT : (s + 1) * ROOT]
            im = out[HALF:, s * ROOT : (s + 1) * ROOT]
            z_hi, z_lo = split(
                jnp.concatenate([re * cos_t + im * sin_t, im * cos_t - re * sin_t], axis=1)
            )
            at = row + (r + s) * HALF
            zbuf[at : at + HALF, 0 : 2 * ROOT] = z_hi
            zbuf[at : at + HALF, 2 * ROOT : 4 * ROOT] = z_lo
            zbuf[at : at + HALF, 4 * ROOT :] = z_hi
    return edge * edge


def squares(left, right):
    out = jnp.dot(left, right, preferred_element_type=jnp.float32)
    return out[:, :ROOT] * out[:, :ROOT] + out[:, ROOT:] * out[:, ROOT:]


def group_sums(lo_ref, hi_ref, right_ref, left_ref, right_on, left_on, per_dev, consts, scratch, put, put_edge):
    window_ref, first_ref, second_ref, twist_ref = consts
    buf, zbuf, ebuf, psum = scratch
    half_len = ROOT * HALF
    block = ROWS * HALF
    lane = lax.broadcasted_iota(jnp.int32, (ROWS, ROOT), 1)
    nyq = []
    for side, own, other, on in ((0, lo_ref, right_ref, right_on), (1, hi_ref, left_ref, left_on)):
        straddle = ((own, half_len), (other, 0)) if side == 0 else ((other, 0), (own, 0))
        first = stage_one(
            ((own, 0), (own, half_len)), window_ref, first_ref, twist_ref, buf, zbuf, ebuf, 0, side * 2 * ROWS
        )
        second = stage_one(
            straddle, window_ref, first_ref, twist_ref, buf, zbuf, ebuf, block, (side * 2 + 1) * ROWS
        )
        nyq.append(first + on * second)
        for r in range(ROWS):
            rows = pl.ds(r * HALF, HALF)
            both = jnp.concatenate([zbuf[rows, :], zbuf[pl.ds(block + r * HALF, HALF), :]], axis=0)
            power = squares(both, second_ref[...])
            psum[r * ROOT + side * HALF : r * ROOT + (side + 1) * HALF, :] = power[:HALF] + on * power[HALF:]
    for r in range(ROWS):
        put(r, jnp.transpose(psum[r * ROOT : (r + 1) * ROOT, :]))
    edge_power = squares(ebuf[...], second_ref[...])
    for side, on in ((0, right_on), (1, left_on)):
        at = side * 2 * ROWS
        mixed = edge_power[at : at + ROWS] + on * edge_power[at + ROWS : at + 2 * ROWS]
        put_edge(side, jnp.where(lane % (2 * per_dev) < per_dev, mixed, jnp.broadcast_to(nyq[side], (ROWS, ROOT))))


def welch_kernel(
    pieces, scale, strain_ref, window_ref, first_ref, second_ref, twist_ref, mirror_ref,
    power_ref, nyquist_ref, mean_ref,
    data, right_half, left_half, sums, edge_rows, edge_sums, from_left, from_right, edge_left, edge_right,
    buf, zbuf, ebuf, psum, channel_sums, channel_from,
    load_sem, halo_send, halo_recv, line_send, line_recv, edge_send, edge_recv, chan_send, chan_recv,
):
    chan, chan_count = lax.axis_index("chan"), lax.axis_size("chan")
    me = lax.axis_index("tm")
    count = lax.axis_size("tm")
    per_dev = HALF // count
    rows = 2 * per_dev
    half_len = ROOT * HALF
    pairs = sums.shape[1]
    groups = pairs // ROWS
    width = pairs // pieces
    has_left, has_right = me > 0, me < count - 1
    right_on, left_on = has_right.astype(jnp.float32), has_left.astype(jnp.float32)

    def block(g, side):
        return pl.ds(pl.multiple_of(side * pairs + g * ROWS, ROWS), ROWS)

    def load(g, side):
        return pltpu.make_async_copy(
            strain_ref.at[block(g, side)], data.at[block(g, side)], load_sem.at[side, g]
        )

    def halo(g, side):
        source = strain_ref.at[block(g, side), pl.ds(side * half_len, half_len)]
        target = (right_half, left_half)[side]
        return pltpu.make_async_remote_copy(
            src_ref=source, dst_ref=target.at[block(g, 0)],
            send_sem=halo_send.at[side, g], recv_sem=halo_recv.at[side, g],
            device_id={"tm": me + (1 if side else -1)}, device_id_type=pl.DeviceIdType.MESH,
        )

    @pl.loop(0, groups)
    def _(g):
        load(g, 0).start()
        load(g, 1).start()

    barrier = pltpu.get_barrier_semaphore()
    for exists, step in ((has_left, -1), (has_right, 1)):
        @pl.when(exists)
        def _():
            pl.semaphore_signal(
                barrier, inc=1, device_id={"tm": me + step}, device_id_type=pl.DeviceIdType.MESH
            )
    for k in range(1, chan_count):
        pl.semaphore_signal(
            barrier, inc=1, device_id={"chan": lax.rem(chan + k, chan_count)},
            device_id_type=pl.DeviceIdType.MESH,
        )
    pl.semaphore_wait(
        barrier, has_left.astype(jnp.int32) + has_right.astype(jnp.int32) + (chan_count - 1)
    )

    @pl.loop(0, groups)
    def _(g):
        for side, exists in ((0, has_left), (1, has_right)):
            @pl.when(exists)
            def _():
                halo(g, side).start()

    edge_rows[...] = jnp.zeros_like(edge_rows)
    for side, exists, ref in ((0, has_right, right_half), (1, has_left, left_half)):
        @pl.when(jnp.logical_not(exists))
        def _():
            ref[...] = jnp.zeros_like(ref)

    def chunk_of(m, side):
        far = lax.rem(m, count - 1)
        return far if side else count - 1 - far

    def sum_part(m, side):
        q = m // (count - 1)
        return sums.at[pl.ds(chunk_of(m, side) * rows, rows), pl.ds(pl.multiple_of(q * width, ROWS), width)]

    def edge_part(m, side):
        return edge_sums.at[pl.ds(chunk_of(m, side) * rows, rows)]

    def line(m, side):
        target = (from_left, from_right)[side]
        return pltpu.make_async_remote_copy(
            src_ref=sum_part(m, side), dst_ref=target.at[m],
            send_sem=line_send.at[side, m], recv_sem=line_recv.at[side, m],
            device_id={"tm": me + (-1 if side else 1)}, device_id_type=pl.DeviceIdType.MESH,
        )

    def edge_line(m, side):
        target = (edge_left, edge_right)[side]
        far = lax.rem(m, count - 1)
        return pltpu.make_async_remote_copy(
            src_ref=edge_part(m, side), dst_ref=target.at[far],
            send_sem=edge_send.at[side, far], recv_sem=edge_recv.at[side, far],
            device_id={"tm": me + (-1 if side else 1)}, device_id_type=pl.DeviceIdType.MESH,
        )

    def take(m, side):
        line(m, side).wait_recv()
        part = sum_part(m, side)
        part[...] = part[...] + (from_left, from_right)[side][m]

        @pl.when(m >= (pieces - 1) * (count - 1))
        def _():
            edge_line(m, side).wait_recv()
            edge = edge_part(m, side)
            edge[...] = edge[...] + (edge_left, edge_right)[side][lax.rem(m, count - 1)]

    messages = (count - 1) * pieces
    hop = 2
    early = max(1, count // 4)

    def place_of(side):
        return count - 1 - me if side else me

    def take_and_send(m, side):
        @pl.when(place_of(side) > 0)
        def _():
            take(m, side)

        line(m, side).start()

        @pl.when(m >= (pieces - 1) * (count - 1))
        def _():
            edge_line(m, side).start()

    @pl.loop(0, groups)
    def _(g):
        load(g, 0).wait()
        load(g, 1).wait()
        for side, exists in ((0, has_right), (1, has_left)):
            @pl.when(exists)
            def _():
                halo(g, side).wait_recv()

        def put(r, value):
            sums[:, g * ROWS + r, :] = value

        def put_edge(side, value):
            edge_rows[block(g, side), :] = value

        group_sums(
            data.at[block(g, 0)], data.at[block(g, 1)], right_half.at[block(g, 0)], left_half.at[block(g, 0)],
            right_on, left_on, per_dev,
            (window_ref, first_ref, second_ref, twist_ref), (buf, zbuf, ebuf, psum), put, put_edge,
        )

        @pl.when(g == groups - 1)
        def _():
            for s in range(edge_sums.shape[1]):
                edge_sums[:, s, :] = jnp.transpose(edge_rows[s * ROOT : (s + 1) * ROOT, :])

        @pl.when(lax.rem(g + 1, groups // pieces) == 0)
        def _():
            q = g // (groups // pieces)
            for side in range(2):
                place = place_of(side)

                @pl.when(place < early)
                def _():
                    @pl.loop(0, count - 1)
                    def _(far):
                        @pl.when(far < count - 1 - place)
                        def _():
                            take_and_send(q * (count - 1) + far, side)

    spread = edge_sums.shape[1]

    @pl.loop(0, messages + hop * (count - 1))
    def _(t):
        for side in range(2):
            place = place_of(side)
            m = t - hop * place

            @pl.when(jnp.logical_and(place >= early, jnp.logical_and(m >= 0, m < messages)))
            def _():
                @pl.when(lax.rem(m, count - 1) < count - 1 - place)
                def _():
                    take_and_send(m, side)

    for side in range(2):
        place = place_of(side)

        @pl.when(place > 0)
        def _():
            @pl.loop(0, pieces)
            def _(q):
                take(q * (count - 1) + (count - 1 - place), side)

    nyquist_ref[...] = edge_sums[me * rows + per_dev] * scale
    for s in range(spread):
        strip = jnp.concatenate(
            [edge_sums[me * rows + j, s : s + 1, :] for j in range(per_dev)]
            + [jnp.zeros((ROOT - per_dev, ROOT), jnp.float32)],
            axis=0,
        )
        edge_rows[s * ROOT : (s + 1) * ROOT, :] = jnp.transpose(strip)
    lanes = lax.broadcasted_iota(jnp.int32, (1, ROOT), 1)
    for j in range(per_dev):
        both = jnp.concatenate([sums[me * rows + j], sums[me * rows + per_dev + j]], axis=1)
        placed = jnp.dot(
            both, mirror_ref[...], precision=lax.Precision.HIGHEST, preferred_element_type=jnp.float32
        )
        factor = jnp.where(jnp.logical_and(lanes == 0, me + j == 0), scale, 2.0 * scale)
        column = jnp.zeros((1, ROOT), jnp.float32)
        for side in range(2):
            middle = edge_rows[side * pairs : (side + 1) * pairs, j : j + 1]
            value = jnp.where(lanes == HALF, middle, placed[:, side * ROOT : (side + 1) * ROOT]) * factor
            power_ref[side * pairs : (side + 1) * pairs, j * ROOT : (j + 1) * ROOT] = value
            column = column + jnp.sum(value, axis=0, keepdims=True)
        channel_sums[j : j + 1, :] = column

    def chan_copy(k):
        return pltpu.make_async_remote_copy(
            src_ref=channel_sums, dst_ref=channel_from.at[k],
            send_sem=chan_send.at[k], recv_sem=chan_recv.at[k],
            device_id={"chan": lax.rem(chan + k, chan_count)}, device_id_type=pl.DeviceIdType.MESH,
        )

    for k in range(1, chan_count):
        chan_copy(k).start()

    @pl.loop(0, groups)
    def _(g):
        for side, exists in ((0, has_left), (1, has_right)):
            @pl.when(exists)
            def _():
                halo(g, side).wait_send()

    @pl.loop(0, messages)
    def _(m):
        for side in range(2):
            place = count - 1 - me if side else me

            @pl.when(lax.rem(m, count - 1) < count - 1 - place)
            def _():
                line(m, side).wait_send()

                @pl.when(m >= (pieces - 1) * (count - 1))
                def _():
                    edge_line(m, side).wait_send()

    channel_from[0] = channel_sums[...]
    for k in range(1, chan_count):
        chan_copy(k).wait()
    total = jnp.zeros_like(channel_sums)
    for source in range(chan_count):
        total = total + channel_from[lax.rem(chan - source + chan_count, chan_count)]
    mean_ref[...] = total * (1.0 / (2 * pairs * chan_count))


def per_device(strain):
    chan_rows, time_width = strain.shape
    seg_len = ROOT * ROOT
    half_len = seg_len // 2
    assert time_width == seg_len and chan_rows % (2 * ROWS) == 0
    tm_count = lax.axis_size("tm")
    segments = 2 * tm_count - 1
    band = half_len // tm_count
    per_dev = HALF // tm_count
    rows = 2 * per_dev
    first_all, second_all, twist, window, mirror, energy = tables(tm_count)
    pairs = chan_rows // 2
    groups = pairs // ROWS
    pieces = 4 if groups % 4 == 0 else 1
    spread = -(-chan_rows // ROOT)
    messages = (tm_count - 1) * pieces
    vmem = pl.BlockSpec(memory_space=pltpu.VMEM)
    f32 = jnp.float32
    power, nyquist, mean_power = pl.pallas_call(
        functools.partial(welch_kernel, pieces, 1.0 / (segments * energy)),
        in_specs=[pl.BlockSpec(memory_space=pl.ANY)] + [vmem] * 5,
        out_specs=[vmem] * 3,
        out_shape=[
            jax.ShapeDtypeStruct((chan_rows, band), f32),
            jax.ShapeDtypeStruct((spread, ROOT), f32),
            jax.ShapeDtypeStruct((per_dev, ROOT), f32),
        ],
        scratch_shapes=[
            pltpu.VMEM((chan_rows, seg_len), f32),
            pltpu.VMEM((pairs, half_len), f32),
            pltpu.VMEM((pairs, half_len), f32),
            pltpu.VMEM((ROOT, pairs, ROOT), f32),
            pltpu.VMEM((spread * ROOT, ROOT), f32),
            pltpu.VMEM((ROOT, spread, ROOT), f32),
            pltpu.VMEM((messages, rows, pairs // pieces, ROOT), f32),
            pltpu.VMEM((messages, rows, pairs // pieces, ROOT), f32),
            pltpu.VMEM((tm_count - 1, rows, spread, ROOT), f32),
            pltpu.VMEM((tm_count - 1, rows, spread, ROOT), f32),
            pltpu.VMEM((ROWS * ROOT, ROOT), f32),
            pltpu.VMEM((2 * ROWS * HALF, 6 * ROOT), jnp.bfloat16),
            pltpu.VMEM((4 * ROWS, 6 * ROOT), jnp.bfloat16),
            pltpu.VMEM((ROWS * ROOT, ROOT), f32),
            pltpu.VMEM((per_dev, ROOT), f32),
            pltpu.VMEM((lax.axis_size("chan"), per_dev, ROOT), f32),
            pltpu.SemaphoreType.DMA((2, groups)),
            pltpu.SemaphoreType.DMA((2, groups)),
            pltpu.SemaphoreType.DMA((2, groups)),
            pltpu.SemaphoreType.DMA((2, messages)),
            pltpu.SemaphoreType.DMA((2, messages)),
            pltpu.SemaphoreType.DMA((2, tm_count - 1)),
            pltpu.SemaphoreType.DMA((2, tm_count - 1)),
            pltpu.SemaphoreType.DMA((lax.axis_size("chan"),)),
            pltpu.SemaphoreType.DMA((lax.axis_size("chan"),)),
        ],
        compiler_params=pltpu.CompilerParams(
            collective_id=0, has_side_effects=True, vmem_limit_bytes=60 * 2**20
        ),
        name="welch",
    )(strain, window, first_all, second_all, twist, mirror)
    return (power, nyquist.reshape(-1)[:chan_rows], mean_power.reshape(-1))


def solution(mesh):
    in_specs = (P("chan", "tm"),)
    out_specs = (P("chan", "tm"), P("chan"), P("tm"))
    return jax.shard_map(
        per_device, mesh=mesh, in_specs=in_specs, out_specs=out_specs, check_vma=False
    )
```
